32 devices in a mesh: dp: 8 (over y, x, core), tensor: 4 (over z).
Axes of the slice: x: 2, y: 2, z: 4, core: 2. Of those that a mesh axis runs over, the one named last changes fastest.
Arguments:
- layer_input: bfloat16 [8192, 2048], P(('dp', 'tensor')), may hold values from -6 to 6
- w_query: bfloat16 [2048, 2048], P('dp', 'tensor'), may hold values from -0.125 to 0.125
- w_key: bfloat16 [2048, 2048], P('dp', 'tensor'), may hold values from -0.125 to 0.125
- w_value: bfloat16 [2048, 2048], P('dp', 'tensor'), may hold values from -0.125 to 0.125
- w_output: bfloat16 [2048, 2048], P('tensor', 'dp'), may hold values from -2 to 2
- w_gate: bfloat16 [2048, 8192], P('dp', 'tensor'), may hold values from -0.125 to 0.125
- w_up: bfloat16 [2048, 8192], P('dp', 'tensor'), may hold values from -0.125 to 0.125
- w_down: bfloat16 [8192, 2048], P('tensor', 'dp'), may hold values from -0.0625 to 0.0625
- cotangent: bfloat16 [8192, 2048], P(('dp', 'tensor')), may hold values from -6 to 6
- lengths: int32 [8], P('dp'), may hold values from 512 to 1024, as said below
Outputs:
- layer_output: bfloat16 [8192, 2048], P(('dp', 'tensor'))
- input_grad: float32 [8192, 2048], P(('dp', 'tensor'))
- grad_query: float32 [2048, 2048], P('dp', 'tensor')
- grad_key: float32 [2048, 2048], P('dp', 'tensor')
- grad_value: float32 [2048, 2048], P('dp', 'tensor')
- grad_output: float32 [2048, 2048], P('tensor', 'dp')
- grad_gate: float32 [2048, 8192], P('dp', 'tensor')
- grad_up: float32 [2048, 8192], P('dp', 'tensor')
- grad_down: float32 [8192, 2048], P('tensor', 'dp')
The draws below stay inside these ranges and needn't reach their ends.
Inputs may be any that keep to these rules, and one draw needn't show every extreme that they name: Slot s holds one sequence in its first lengths[s] rows, the rest is padding; every draw has a slot of exactly 1024 and one of exactly 512.
All inputs are finite; a program needn't handle non-finite values.
Results may differ from the reference program's by a relative error of at most 0.019.
Values may be sent and summed in bfloat16 or wider, within the bound.
A program may use at most 192 MiB of HBM per device.

```python
import math
import jax
import jax.numpy as jnp
from jax import lax

D = 2048
HEADS = 16
HD = 128
FF = 8192
SLOT = 1024
QB = 512
LEAST = 512
SLOTS = 8
TOKENS = 8192


def draw_lengths(key, part):
    key_one = jax.random.fold_in(key, 11)
    key_two = jax.random.fold_in(key, 12)
    key_three = jax.random.fold_in(key, 13)
    values = jax.random.randint(key_one, (SLOTS,), LEAST, SLOT + 1)
    full_at = jax.random.randint(key_two, (), 0, SLOTS)
    least_at = (full_at + 1 + jax.random.randint(key_three, (), 0, SLOTS - 1)) % SLOTS
    values = values.at[full_at].set(SLOT)
    values = values.at[least_at].set(LEAST)
    return values.astype(jnp.int32)


def raised(values, rng, source, target, parts, factor):
    def block_of(axis_at):
        return (jnp.arange(values.shape[axis_at]) // (values.shape[axis_at] // parts)).reshape((-1,) + (1,) * (values.ndim - 1 - axis_at))

    one_side = jax.random.permutation(rng, parts)[block_of(target)]
    second = (block_of(target) + parts // 2) % parts
    return jnp.where((block_of(source) == one_side) | (block_of(source) == second), factor * values, values)


def level_of(stream_key, dims, pieces, smallest, largest):
    loudness, own = 1.0, jax.random.fold_in(stream_key, 6)
    for dim, blocks in pieces:
        draws = jnp.exp(jax.random.uniform(jax.random.fold_in(own, dim), (blocks,), jnp.float32, smallest / len(pieces), largest / len(pieces)))
        loudness = loudness * jnp.repeat(draws, dims[dim] // blocks).reshape([-1 if axis == dim else 1 for axis in range(len(dims))])
    return loudness


def centred(rng, extent, deviation, reach, shards=(), held_as=jnp.bfloat16):
    drawn = deviation * jax.random.normal(rng, extent, jnp.float32)
    if shards:
        drawn = drawn * level_of(rng, extent, shards, -0.22, 0.18)
    return jnp.clip(drawn, -reach, reach).astype(held_as)


def gaussian_with(stream_key, shape, scale, reach, shards, heavy, kind=jnp.bfloat16):
    result = scale * jax.random.normal(stream_key, shape, jnp.float32)
    if shards:
        result = result * level_of(stream_key, shape, shards, -0.22, 0.18)
    return jnp.clip(raised(result, jax.random.fold_in(stream_key, 3), *heavy), -reach, reach).astype(kind)


def setup_inputs(seed: int = 0) -> dict:
    key_list = jax.random.split(jax.random.key(seed), 11)
    layer_input = centred(key_list[0], (TOKENS, D), 1.0, 6.0, ((0, 32),))
    w_query = centred(key_list[1], (D, D), D ** -0.5, 0.125, ((0, 8), (1, 4)))
    w_key = centred(key_list[2], (D, D), D ** -0.5, 0.125, ((0, 8), (1, 4)))
    w_value = centred(key_list[3], (D, D), D ** -0.5, 0.125, ((0, 8), (1, 4)))
    w_output = centred(key_list[4], (D, D), (max(D // 256, 1)) ** -0.5, 2.0, ((0, 4), (1, 8)))
    w_gate = centred(key_list[5], (D, FF), D ** -0.5, 0.125, ((0, 8), (1, 4)))
    w_up = centred(key_list[6], (D, FF), D ** -0.5, 0.125, ((0, 8), (1, 4)))
    w_down = centred(key_list[7], (FF, D), FF ** -0.5, 0.0625, ((0, 4), (1, 8)))
    cotangent = gaussian_with(key_list[8], (TOKENS, D), 1.0, 6.0, ((0, 32),), (0, 1, 32, 2.75))
    lengths = draw_lengths(jax.random.fold_in(key_list[10], 71), 0)
    return dict(layer_input=layer_input, w_query=w_query, w_key=w_key, w_value=w_value, w_output=w_output, w_gate=w_gate, w_up=w_up, w_down=w_down, cotangent=cotangent, lengths=lengths)


EPSILON = 1e-05
THETA = 10000.0
MASKED = -1e+30

@jax.custom_vjp
def low(v):
    return lax.optimization_barrier(v.astype(jnp.bfloat16)).astype(jnp.float32)

@jax.custom_vjp
def low_back(v):
    return v

def low_keep(v):
    return (low(v), None)

def low_pass(kept, grad):
    return (grad,)

def back_keep(v):
    return (v, None)

def back_low(kept, grad):
    return (low(grad),)
low.defvjp(low_keep, low_pass)
low_back.defvjp(back_keep, back_low)

def normalize(values):
    center = values - lax.optimization_barrier(jnp.mean(values, axis=-1, keepdims=True))
    spread = lax.optimization_barrier(jnp.mean(center * center, axis=-1, keepdims=True))
    return center * lax.rsqrt(spread + EPSILON)

def rotary(values, cos_table, sin_table):
    midway = values.shape[-1] // 2
    turned = jnp.concatenate([-values[..., midway:], values[..., :midway]], axis=-1)
    return values * cos_table + turned * sin_table

def rope_tables(row_count, head_size):
    midway = head_size // 2
    frequency = THETA ** (-(jnp.arange(midway, dtype=jnp.float32) * 2.0 / head_size))
    phases = jnp.arange(row_count, dtype=jnp.int32).astype(jnp.float32)[:, None] * frequency[None, :]
    phases = jnp.concatenate([phases, phases], axis=-1)
    return (jnp.cos(phases)[:, None, :], jnp.sin(phases)[:, None, :])

def exact_product(first_op, second_op):
    return jnp.dot(first_op, second_op, precision=lax.Precision.HIGHEST, preferred_element_type=jnp.float32)

def layer(row_input, w_query, w_key, w_value, w_output, w_gate, w_up, w_down, seq_length):
    scale = 1.0 / math.sqrt(HD)
    positions = jnp.arange(SLOT, dtype=jnp.int32)
    cos_table, sin_table = rope_tables(SLOT, HD)
    normed_one = low(normalize(row_input))
    query_raw = low_back(exact_product(normed_one, w_query)).reshape(SLOT, HEADS, HD)
    key_raw = low_back(exact_product(normed_one, w_key)).reshape(SLOT, HEADS, HD)
    query_low = low(rotary(query_raw, cos_table, sin_table))
    key_rot = low(rotary(key_raw, cos_table, sin_table))
    values_low = low(low_back(exact_product(normed_one, w_value))).reshape(SLOT, HEADS, HD)
    key_valid = positions < seq_length

    def block_attend(offset):
        query_block = lax.dynamic_slice_in_dim(query_low, offset, QB, 0)
        raw_scores = jnp.einsum('qhe,khe->hqk', query_block, key_rot, precision=lax.Precision.HIGHEST) * scale
        raw_scores = low_back(raw_scores)
        query_pos = offset + jnp.arange(QB, dtype=jnp.int32)
        allowed = (positions[None, :] <= query_pos[:, None]) & key_valid[None, :]
        masked = jnp.where(allowed[None], raw_scores, MASKED)
        probs = low(jax.nn.softmax(masked, axis=-1))
        return jnp.einsum('hqk,khe->qhe', probs, values_low, precision=lax.Precision.HIGHEST)
    offsets = jnp.arange(SLOT // QB, dtype=jnp.int32) * QB
    contexts = lax.map(jax.checkpoint(block_attend), offsets)
    context_low = low(low_back(contexts.reshape(SLOT, HEADS * HD)))
    attended = row_input + low_back(exact_product(context_low, w_output))
    normed_two = low(normalize(attended))
    gate_pre = low_back(exact_product(normed_two, w_gate))
    up_pre = low_back(exact_product(normed_two, w_up))
    hidden = low(jax.nn.silu(gate_pre) * up_pre)
    return attended + low_back(exact_product(hidden, w_down))

def reference(layer_input, w_query, w_key, w_value, w_output, w_gate, w_up, w_down, cotangent, lengths):
    weights = (w_query.astype(jnp.float32), w_key.astype(jnp.float32), w_value.astype(jnp.float32), w_output.astype(jnp.float32), w_gate.astype(jnp.float32), w_up.astype(jnp.float32), w_down.astype(jnp.float32))
    slot_inputs = layer_input.astype(jnp.float32).reshape(SLOTS, SLOT, D)
    slot_cots = cotangent.astype(jnp.float32).reshape(SLOTS, SLOT, D)

    def slot_step(running, item):
        row_input, row_cot, seq_length = item

        def forward(inputs, wq_in, wk_in, wv_in, wo_in, wg_in, wu_in, wd_in):
            return layer(inputs, wq_in, wk_in, wv_in, wo_in, wg_in, wu_in, wd_in, seq_length)
        result_rows, pullback = jax.vjp(forward, row_input, *weights)
        keep_rows = (jnp.arange(SLOT, dtype=jnp.int32) < seq_length).astype(jnp.float32)[:, None]
        grads = pullback(row_cot * keep_rows)
        running = tuple((acc + part_grad for acc, part_grad in zip(running, grads[1:])))
        return (running, (result_rows, grads[0]))
    zeros_init = tuple((jnp.zeros_like(weight_arr) for weight_arr in weights))
    running, (result_all, input_all) = lax.scan(slot_step, zeros_init, (slot_inputs, slot_cots, lengths))
    layer_output = result_all.reshape(TOKENS, D).astype(jnp.bfloat16)
    input_grad = input_all.reshape(TOKENS, D)
    return (layer_output, input_grad, running[0], running[1], running[2], running[3], running[4], running[5], running[6])
```

```python
import math

import jax
import jax.numpy as jnp
from jax import lax
from jax.sharding import PartitionSpec as P

HD = 128
QB = 512

EPSILON = 1e-05
THETA = 10000.0
MASKED = -1e30


def normalize(values):
    center = values - jnp.mean(values, axis=-1, keepdims=True)
    spread = jnp.mean(center * center, axis=-1, keepdims=True)
    return center * lax.rsqrt(spread + EPSILON)


def rotary(values, cos_table, sin_table):
    midway = values.shape[-1] // 2
    turned = jnp.concatenate([-values[..., midway:], values[..., :midway]], axis=-1)
    return values * cos_table + turned * sin_table


def rope_tables(row_count, head_size):
    midway = head_size // 2
    frequency = THETA ** (-(jnp.arange(midway, dtype=jnp.float32) * 2.0 / head_size))
    phases = (
        jnp.arange(row_count, dtype=jnp.int32).astype(jnp.float32)[:, None] * frequency[None, :]
    )
    phases = jnp.concatenate([phases, phases], axis=-1)
    return (jnp.cos(phases), jnp.sin(phases))


def plain_product(first_op, second_op):
    return jnp.dot(first_op, second_op, preferred_element_type=jnp.float32)


def left_product(first_op, second_op):
    return lax.dot_general(
        first_op, second_op, (((0,), (0,)), ((), ())), preferred_element_type=jnp.float32
    )


def right_product(first_op, second_op):
    return lax.dot_general(
        first_op, second_op, (((1,), (1,)), ((), ())), preferred_element_type=jnp.float32
    )


def gated(gate_in, upward):
    return jax.nn.silu(gate_in) * upward


def low(values):
    return values.astype(jnp.bfloat16)


def wide(values):
    return values.astype(jnp.float32)


def tied(value, *deps):
    return lax.optimization_barrier((value,) + deps)[0]


def flip(value, bit, count):
    return lax.ppermute(value, "dp", [(i, i ^ bit) for i in range(count)])


def step_to(value, shift, count):
    return lax.ppermute(value, "tensor", [(i, (i + shift) % count) for i in range(count)])


def far_bits(count):
    bits, bit = [], 2
    while bit < count:
        bits.append(bit)
        bit *= 2
    return bits


def spread_blocks(shard, axis, count):
    half = shard.shape[axis] // 2
    bits = far_bits(count)
    paths = []
    for at, order in ((0, bits), (half, bits[::-1])):
        have = {0: lax.slice_in_dim(shard, at, at + half, axis=axis)}
        for bit in order:
            have.update({k ^ bit: flip(v, bit, count) for k, v in have.items()})
        paths.append(have)
    near = jnp.concatenate(
        [paths[side][2 * p] for p in range(count // 2) for side in (0, 1)], axis=axis
    )
    other = flip(near, 1, count)
    return jnp.concatenate([near, other], axis=axis)


def collect_blocks(total, axis, count):
    width = total.shape[axis] // count
    half = width // 2
    middle = total.shape[axis] // 2
    near = lax.slice_in_dim(total, 0, middle, axis=axis)
    other = lax.slice_in_dim(total, middle, 2 * middle, axis=axis)
    near = wide(near) + wide(flip(low(other), 1, count))
    bits = far_bits(count)
    sides = []
    for at, order in ((0, bits), (half, bits[::-1])):
        have = {
            2 * p: lax.slice_in_dim(near, p * width + at, p * width + at + half, axis=axis)
            for p in range(count // 2)
        }
        for bit in order:
            keep = [k for k in have if not k & bit]
            have = {k: have[k] + wide(flip(low(have[k ^ bit]), bit, count)) for k in keep}
        sides.append(have[0])
    return jnp.concatenate(sides, axis=axis)


def ring_gather(rows, count):
    half = rows.shape[0] // 2
    blocks = {0: rows}
    fore = back = rows
    for step in range(1, count // 2):
        fore = step_to(fore, 1, count)
        back = step_to(back, -1, count)
        blocks[count - step] = fore
        blocks[step] = back
    fore = step_to(fore[:half], 1, count)
    back = step_to(back[half:], -1, count)
    blocks[count // 2] = jnp.concatenate([fore, back], axis=0)
    return jnp.concatenate([blocks[j] for j in range(count)], axis=0)


def ring_collect(total, count):
    size = total.shape[0] // count
    half = size // 2
    block = lambda j: wide(total[j * size : (j + 1) * size])
    middle = count // 2
    opposite = block(middle)
    fore = step_to(low(opposite[:half]), 1, count)
    back = step_to(low(opposite[half:]), -1, count)
    if middle == 1:
        return block(0) + jnp.concatenate([wide(fore), wide(back)], axis=0)
    for step in range(middle - 1, 0, -1):
        ahead, behind = block(step), block(count - step)
        if step == middle - 1:
            ahead = jnp.concatenate([ahead[:half] + wide(fore), ahead[half:]], axis=0)
            behind = jnp.concatenate([behind[:half], behind[half:] + wide(back)], axis=0)
        else:
            ahead, behind = ahead + wide(fore), behind + wide(back)
        fore = step_to(low(ahead), 1, count)
        back = step_to(low(behind), -1, count)
    return block(0) + wide(fore) + wide(back)


def shards(
    layer_input, w_query, w_key, w_value, w_output, w_gate, w_up, w_down, cotangent, lengths
):
    tensor_parts = lax.axis_size("tensor")
    tensor_index = lax.axis_index("tensor")
    dp_parts = lax.axis_size("dp")
    dp_index = lax.axis_index("dp")
    rows_dev, width = layer_input.shape
    slot_rows = rows_dev * tensor_parts
    head_width = w_query.shape[1]
    heads_dev = head_width // HD
    seq_length = lengths[0]
    scale = 1.0 / math.sqrt(HD)
    block = width // dp_parts
    half_parts = dp_parts // 2

    def to_relative(values):
        order = [2 * p for p in range(half_parts)] + [2 * p + 1 for p in range(half_parts)]
        return jnp.concatenate(
            [
                lax.dynamic_slice_in_dim(values, (dp_index ^ k) * block, block, 1)
                for k in order
            ],
            axis=1,
        )

    def from_relative(values):
        pieces = []
        for j in range(dp_parts):
            k = dp_index ^ j
            place = (k & 1) * half_parts + (k >> 1)
            pieces.append(lax.dynamic_slice_in_dim(values, place * block, block, 1))
        return jnp.concatenate(pieces, axis=1)

    row_ids = tensor_index * rows_dev + jnp.arange(rows_dev, dtype=jnp.int32)
    positions = (tensor_index * rows_dev + jnp.arange(slot_rows, dtype=jnp.int32)) % slot_rows
    key_valid = positions < seq_length
    cos_table, sin_table = rope_tables(slot_rows, HD)
    start = tensor_index * rows_dev

    def rotated_rows(table):
        return lax.dynamic_slice_in_dim(
            jnp.concatenate([table, table], axis=0), start, slot_rows, 0
        )[:, None, :]

    cos_table, sin_table = rotated_rows(cos_table), rotated_rows(sin_table)

    full_qkv = spread_blocks(jnp.concatenate([w_query, w_key, w_value], axis=1), 0, dp_parts)
    full_output = spread_blocks(tied(w_output, full_qkv), 1, dp_parts)
    full_gate = spread_blocks(tied(w_gate, full_output), 0, dp_parts)
    full_up = spread_blocks(tied(w_up, full_gate), 0, dp_parts)
    full_down = spread_blocks(tied(w_down, full_up), 1, dp_parts)

    inputs = wide(to_relative(layer_input))
    keep_rows = (row_ids < seq_length).astype(jnp.float32)[:, None]
    grad_final = wide(to_relative(cotangent)) * keep_rows

    rows_one = ring_gather(low(normalize(inputs)), tensor_parts)
    cot_rows = ring_gather(tied(low(grad_final), rows_one), tensor_parts)

    qkv = plain_product(rows_one, full_qkv)
    query_raw = qkv[:, :head_width].reshape(slot_rows, heads_dev, HD)
    key_raw = qkv[:, head_width : 2 * head_width].reshape(slot_rows, heads_dev, HD)
    query_low = low(rotary(query_raw, cos_table, sin_table))
    key_rot = low(rotary(key_raw, cos_table, sin_table))
    values_low = low(qkv[:, 2 * head_width :]).reshape(slot_rows, heads_dev, HD)

    offsets = jnp.arange(slot_rows // QB, dtype=jnp.int32) * QB

    def masked_scores(offset):
        query_block = lax.dynamic_slice_in_dim(query_low, offset, QB, 0)
        raw_scores = (
            jnp.einsum("qhe,khe->hqk", query_block, key_rot, preferred_element_type=jnp.float32)
            * scale
        )
        query_pos = lax.dynamic_slice_in_dim(positions, offset, QB, 0)
        allowed = (positions[None, :] <= query_pos[:, None]) & key_valid[None, :]
        return jnp.where(allowed[None], raw_scores, MASKED)

    def attend(offset):
        scores = masked_scores(offset)
        highest = jnp.max(scores, axis=-1, keepdims=True)
        unscaled = jnp.exp(scores - highest)
        summed = jnp.sum(unscaled, axis=-1, keepdims=True)
        prob_low = (unscaled / summed).astype(jnp.bfloat16)
        context = jnp.einsum(
            "hqk,khe->qhe", prob_low, values_low, preferred_element_type=jnp.float32
        )
        return (context, (highest + jnp.log(summed))[..., 0])

    contexts, log_sums = lax.map(attend, offsets)
    context_low = contexts.reshape(slot_rows, head_width).astype(jnp.bfloat16)
    attended = inputs + ring_collect(plain_product(context_low, full_output), tensor_parts)
    rows_two = ring_gather(low(normalize(attended)), tensor_parts)
    gate_pre = plain_product(rows_two, full_gate)
    up_pre = plain_product(rows_two, full_up)
    hidden = gated(gate_pre, up_pre).astype(jnp.bfloat16)

    grad_hidden = right_product(cot_rows, full_down)
    gate_pull = jax.vjp(gated, gate_pre, up_pre)[1]
    grad_gate_pre, grad_up_pre = gate_pull(grad_hidden)
    gate_low = grad_gate_pre.astype(jnp.bfloat16)
    upper_low = grad_up_pre.astype(jnp.bfloat16)
    grad_normed_two = ring_collect(
        right_product(gate_low, full_gate) + right_product(upper_low, full_up), tensor_parts
    )
    norm_pull_two = jax.vjp(normalize, attended)[1]
    grad_attended = grad_final + norm_pull_two(grad_normed_two)[0]
    attn_cot = ring_gather(low(grad_attended), tensor_parts)

    result_rows = attended + ring_collect(plain_product(hidden, full_down), tensor_parts)
    layer_output = from_relative(result_rows.astype(jnp.bfloat16))

    grad_down = collect_blocks(left_product(hidden, cot_rows), 1, dp_parts)
    grad_gate = collect_blocks(left_product(rows_two, gate_low), 0, dp_parts)
    grad_up = collect_blocks(left_product(rows_two, upper_low), 0, dp_parts)

    grad_output = collect_blocks(left_product(context_low, attn_cot), 1, dp_parts)
    grad_context = low(right_product(attn_cot, full_output)).reshape(slot_rows, heads_dev, HD)

    def attend_back(carry, item):
        key_sum, value_sum = carry
        offset, log_block = item
        scores = masked_scores(offset)
        query_block = lax.dynamic_slice_in_dim(query_low, offset, QB, 0)
        grad_block = lax.dynamic_slice_in_dim(grad_context, offset, QB, 0)
        probs = jnp.exp(scores - log_block[..., None])
        grad_probs = jnp.einsum(
            "qhe,khe->hqk", grad_block, values_low, preferred_element_type=jnp.float32
        )
        inner_sum = jnp.sum(probs * grad_probs, axis=-1, keepdims=True)
        grad_scores = (probs * (grad_probs - inner_sum)).astype(jnp.bfloat16)
        query_part = (
            jnp.einsum("hqk,khe->qhe", grad_scores, key_rot, preferred_element_type=jnp.float32)
            * scale
        )
        key_sum = (
            key_sum
            + jnp.einsum(
                "hqk,qhe->khe", grad_scores, query_block, preferred_element_type=jnp.float32
            )
            * scale
        )
        value_sum = value_sum + jnp.einsum(
            "hqk,qhe->khe",
            probs.astype(jnp.bfloat16),
            grad_block,
            preferred_element_type=jnp.float32,
        )
        return ((key_sum, value_sum), query_part)

    zero_rows = jnp.zeros((slot_rows, heads_dev, HD), jnp.float32)
    (key_sum, value_sum), query_parts = lax.scan(
        attend_back, (zero_rows, zero_rows), (offsets, log_sums)
    )
    grad_query_rot = query_parts.reshape(slot_rows, heads_dev, HD)
    rope_pull = jax.vjp(lambda inner: rotary(inner, cos_table, sin_table), query_raw)[1]
    grad_qkv_low = jnp.concatenate(
        [
            low(rope_pull(grad_query_rot)[0].reshape(slot_rows, head_width)),
            low(rope_pull(key_sum)[0].reshape(slot_rows, head_width)),
            low(value_sum.reshape(slot_rows, head_width)),
        ],
        axis=1,
    )
    grad_normed_one = ring_collect(right_product(grad_qkv_low, full_qkv), tensor_parts)
    grad_qkv = collect_blocks(left_product(rows_one, grad_qkv_low), 0, dp_parts)
    norm_pull_one = jax.vjp(normalize, inputs)[1]
    input_grad = from_relative(grad_attended + norm_pull_one(grad_normed_one)[0])
    return (
        layer_output,
        input_grad,
        grad_qkv[:, :head_width],
        grad_qkv[:, head_width : 2 * head_width],
        grad_qkv[:, 2 * head_width :],
        grad_output,
        grad_gate,
        grad_up,
        grad_down,
    )


def solution(mesh):
    return jax.shard_map(
        shards,
        mesh=mesh,
        in_specs=(
            P(("dp", "tensor"), None),
            P("dp", "tensor"),
            P("dp", "tensor"),
            P("dp", "tensor"),
            P("tensor", "dp"),
            P("dp", "tensor"),
            P("dp", "tensor"),
            P("tensor", "dp"),
            P(("dp", "tensor"), None),
            P("dp"),
        ),
        out_specs=(
            P(("dp", "tensor"), None),
            P(("dp", "tensor"), None),
            P("dp", "tensor"),
            P("dp", "tensor"),
            P("dp", "tensor"),
            P("tensor", "dp"),
            P("dp", "tensor"),
            P("dp", "tensor"),
            P("tensor", "dp"),
        ),
        check_vma=False,
    )
```

```python
import math

import jax
import jax.numpy as jnp
from jax import lax
from jax.experimental import pallas as pl
from jax.experimental.pallas import tpu as pltpu
from jax.sharding import PartitionSpec as P


HD = 128
QB = 256

EPSILON = 1e-05
THETA = 10000.0
MASKED = -1e30


def turn(values, cos, signed_sin):
    return values * cos + pltpu.roll(values, HD // 2, 1) * signed_sin


def turn_back(values, cos, signed_sin):
    return values * cos - pltpu.roll(values, HD // 2, 1) * signed_sin


def block_mask(at, length):
    end = at + QB
    rows = at + lax.broadcasted_iota(jnp.int32, (QB, end), 0)
    columns = lax.broadcasted_iota(jnp.int32, (QB, end), 1)
    return (columns <= rows) & (columns < length)


def attend_kernel(length_ref, q_ref, k_ref, v_ref, cos_ref, sin_ref, out_ref, ql_ref, kl_ref, vl_ref, log_ref):
    length = length_ref[0]
    cos, sin = cos_ref[...], sin_ref[...]
    ql_ref[...] = turn(q_ref[...], cos, sin).astype(jnp.bfloat16)
    kl_ref[...] = turn(k_ref[...], cos, sin).astype(jnp.bfloat16)
    vl_ref[...] = v_ref[...].astype(jnp.bfloat16)
    for at in range(0, q_ref.shape[0], QB):
        end = at + QB
        scores = right_product(ql_ref[at:end, :], kl_ref[:end, :]) * (1.0 / math.sqrt(HD))
        scores = jnp.where(block_mask(at, length), scores, MASKED)
        highest = jnp.max(scores, axis=-1, keepdims=True)
        unscaled = jnp.exp(scores - highest)
        summed = jnp.sum(unscaled, axis=-1, keepdims=True)
        prob = (unscaled / summed).astype(jnp.bfloat16)
        out_ref[at:end, :] = plain_product(prob, vl_ref[:end, :]).astype(jnp.bfloat16)
        log_ref[0, at:end, :] = highest + jnp.log(summed)


def attend_back_kernel(length_ref, q_ref, k_ref, v_ref, g_ref, log_ref, cos_ref, sin_ref, gq_ref, gk_ref, gv_ref, key_sum, value_sum):
    length = length_ref[0]
    scale = 1.0 / math.sqrt(HD)
    cos, sin = cos_ref[...], sin_ref[...]
    key_sum[...] = jnp.zeros_like(key_sum)
    value_sum[...] = jnp.zeros_like(value_sum)
    for at in range(0, q_ref.shape[0], QB):
        end = at + QB
        query, grad = q_ref[at:end, :], g_ref[at:end, :]
        scores = right_product(query, k_ref[:end, :]) * scale
        scores = jnp.where(block_mask(at, length), scores, MASKED)
        probs = jnp.exp(scores - log_ref[0, at:end, :])
        grad_probs = right_product(grad, v_ref[:end, :])
        inner = jnp.sum(probs * grad_probs, axis=-1, keepdims=True)
        grad_scores = (probs * (grad_probs - inner)).astype(jnp.bfloat16)
        value_sum[:end, :] += left_product(probs.astype(jnp.bfloat16), grad)
        key_sum[:end, :] += left_product(grad_scores, query)
        grad_query = plain_product(grad_scores, k_ref[:end, :]) * scale
        gq_ref[at:end, :] = turn_back(grad_query, cos[at:end, :], sin[at:end, :]).astype(
            jnp.bfloat16
        )
    gk_ref[...] = turn_back(key_sum[...] * scale, cos, sin).astype(jnp.bfloat16)
    gv_ref[...] = value_sum[...].astype(jnp.bfloat16)


def head_spec(rows, first=0):
    return pl.BlockSpec((rows, HD), lambda h: (0, first + h))


def table_spec(rows):
    return pl.BlockSpec((rows, HD), lambda h: (0, 0))


def attend(lengths, qkv, cos, sin):
    rows, columns = qkv.shape
    heads = columns // (3 * HD)
    low_rows = jax.ShapeDtypeStruct((rows, heads * HD), jnp.bfloat16)
    log_spec = pl.BlockSpec((1, rows, 1), lambda h: (h, 0, 0))
    return pl.pallas_call(
        attend_kernel,
        grid=(heads,),
        in_specs=[pl.BlockSpec(memory_space=pltpu.SMEM)]
        + [head_spec(rows, first) for first in (0, heads, 2 * heads)]
        + [table_spec(rows)] * 2,
        out_specs=[head_spec(rows)] * 4 + [log_spec],
        out_shape=[low_rows] * 4 + [jax.ShapeDtypeStruct((heads, rows, 1), jnp.float32)],
        cost_estimate=pl.CostEstimate(
            flops=4 * rows * rows * heads * HD,
            bytes_accessed=12 * rows * heads * HD,
            transcendentals=rows * rows * heads,
        ),
    )(lengths, qkv, qkv, qkv, cos, sin)


def attend_back(lengths, query, key, value, grad, logs, cos, sin):
    rows, columns = query.shape
    heads = columns // HD
    low_rows = jax.ShapeDtypeStruct((rows, columns), jnp.bfloat16)
    log_spec = pl.BlockSpec((1, rows, 1), lambda h: (h, 0, 0))
    return pl.pallas_call(
        attend_back_kernel,
        grid=(heads,),
        in_specs=[pl.BlockSpec(memory_space=pltpu.SMEM)]
        + [head_spec(rows)] * 4
        + [log_spec]
        + [table_spec(rows)] * 2,
        out_specs=[head_spec(rows)] * 3,
        out_shape=[low_rows] * 3,
        scratch_shapes=[pltpu.VMEM((rows, HD), jnp.float32)] * 2,
        cost_estimate=pl.CostEstimate(
            flops=10 * rows * rows * columns,
            bytes_accessed=16 * rows * columns,
            transcendentals=rows * rows * heads,
        ),
    )(lengths, query, key, value, grad, logs, cos, sin)


def normalize(values):
    center = values - jnp.mean(values, axis=-1, keepdims=True)
    spread = jnp.mean(center * center, axis=-1, keepdims=True)
    return center * lax.rsqrt(spread + EPSILON)


def rope_tables(row_count, head_size):
    midway = head_size // 2
    frequency = THETA ** (-(jnp.arange(midway, dtype=jnp.float32) * 2.0 / head_size))
    phases = (
        jnp.arange(row_count, dtype=jnp.int32).astype(jnp.float32)[:, None] * frequency[None, :]
    )
    cos, sin = jnp.cos(phases), jnp.sin(phases)
    return jnp.concatenate([cos, cos], axis=-1), jnp.concatenate([-sin, sin], axis=-1)


def plain_product(first_op, second_op):
    return jnp.dot(first_op, second_op, preferred_element_type=jnp.float32)


def left_product(first_op, second_op):
    return lax.dot_general(
        first_op, second_op, (((0,), (0,)), ((), ())), preferred_element_type=jnp.float32
    )


def right_product(first_op, second_op):
    return lax.dot_general(
        first_op, second_op, (((1,), (1,)), ((), ())), preferred_element_type=jnp.float32
    )


def gated(gate_in, upward):
    return jax.nn.silu(gate_in) * upward


def low(values):
    return values.astype(jnp.bfloat16)


def wide(values):
    return values.astype(jnp.float32)


def tied(value, *deps):
    return lax.optimization_barrier((value,) + deps)[0]


def flip(value, bit, count):
    return lax.ppermute(value, "dp", [(i, i ^ bit) for i in range(count)])


def spread_blocks(shard, count, cuts):
    pieces = [shard] + [flip(shard, k, count) for k in range(2, count, 2)]
    near = jnp.concatenate(pieces, axis=0)
    other = flip(near, 1, count)
    return [
        jnp.concatenate([near[:, at:to], other[:, at:to]], axis=0)
        for at, to in zip(cuts[:-1], cuts[1:])
    ]


def collect_blocks(total, count):
    middle = total.shape[0] // 2
    width = total.shape[0] // count
    received = flip(total[middle:], 1, count)
    part = lambda p: wide(total[p * width : (p + 1) * width]) + wide(
        received[p * width : (p + 1) * width]
    )
    sent = [flip(low(part(p)), 2 * p, count) for p in range(1, count // 2)]
    result = part(0)
    for piece in sent:
        result = result + wide(piece)
    return result


def tensor_gather(rows):
    return lax.all_gather(rows, "tensor", axis=0, tiled=True)


def tensor_collect(total):
    total = low(total)
    return wide(lax.psum_scatter(total, "tensor", scatter_dimension=0, tiled=True))


def shards(
    layer_input, w_query, w_key, w_value, w_output, w_gate, w_up, w_down, cotangent, lengths
):
    tensor_parts = lax.axis_size("tensor")
    tensor_index = lax.axis_index("tensor")
    dp_parts = lax.axis_size("dp")
    dp_index = lax.axis_index("dp")
    rows_dev, width = layer_input.shape
    slot_rows = rows_dev * tensor_parts
    head_width = w_query.shape[1]
    seq_length = lengths[0]
    block = width // dp_parts
    half_parts = dp_parts // 2

    def to_relative(values):
        order = [2 * p for p in range(half_parts)] + [2 * p + 1 for p in range(half_parts)]
        return jnp.concatenate(
            [
                lax.dynamic_slice_in_dim(values, (dp_index ^ k) * block, block, 1)
                for k in order
            ],
            axis=1,
        )

    def from_relative(values):
        pieces = []
        for j in range(dp_parts):
            k = dp_index ^ j
            place = (k & 1) * half_parts + (k >> 1)
            pieces.append(lax.dynamic_slice_in_dim(values, place * block, block, 1))
        return jnp.concatenate(pieces, axis=1)

    row_ids = tensor_index * rows_dev + jnp.arange(rows_dev, dtype=jnp.int32)
    cos_table, sin_table = rope_tables(slot_rows, HD)

    ff_dev = w_gate.shape[1]
    first_group = jnp.concatenate([w_query, w_key, w_value, w_output.T], axis=1)
    second_group = jnp.concatenate([w_gate, w_up, w_down.T], axis=1)
    full_qkv, full_output = spread_blocks(
        first_group, dp_parts, (0, 3 * head_width, 4 * head_width)
    )
    full_gate, full_up, full_down = spread_blocks(
        second_group, dp_parts, (0, ff_dev, 2 * ff_dev, 3 * ff_dev)
    )

    inputs = wide(to_relative(layer_input))
    keep_rows = (row_ids < seq_length).astype(jnp.float32)[:, None]
    grad_final = wide(to_relative(cotangent)) * keep_rows

    rows_one = tensor_gather(low(normalize(inputs)))
    cot_rows = tensor_gather(tied(low(grad_final), rows_one))

    qkv = plain_product(rows_one, full_qkv)
    context_low, query_low, key_low, values_low, logs = attend(lengths, qkv, cos_table, sin_table)
    attended = inputs + tensor_collect(right_product(context_low, full_output))
    rows_two = tensor_gather(low(normalize(attended)))
    grad_hidden = plain_product(cot_rows, full_down)
    gate_pre = plain_product(rows_two, full_gate)
    up_pre = plain_product(rows_two, full_up)
    hidden = gated(gate_pre, up_pre).astype(jnp.bfloat16)
    gate_pull = jax.vjp(gated, gate_pre, up_pre)[1]
    grad_gate_pre, grad_up_pre = gate_pull(grad_hidden)
    gate_low = grad_gate_pre.astype(jnp.bfloat16)
    upper_low = grad_up_pre.astype(jnp.bfloat16)
    grad_normed_two = tensor_collect(
        right_product(gate_low, full_gate) + right_product(upper_low, full_up)
    )
    norm_pull_two = jax.vjp(normalize, attended)[1]
    grad_attended = grad_final + norm_pull_two(grad_normed_two)[0]
    attn_cot = tensor_gather(low(grad_attended))

    down_part = low(right_product(hidden, full_down))
    result_rows = attended + tensor_collect(down_part)
    layer_output = from_relative(result_rows.astype(jnp.bfloat16))

    total_down = low(left_product(cot_rows, hidden))
    grad_down = collect_blocks(total_down, dp_parts).T
    total_gate = low(left_product(rows_two, gate_low))
    grad_gate = collect_blocks(total_gate, dp_parts)
    total_up = low(left_product(rows_two, upper_low))
    grad_up = collect_blocks(total_up, dp_parts)

    grad_context = low(plain_product(attn_cot, full_output))
    total_output = low(left_product(attn_cot, context_low))
    grad_output = collect_blocks(total_output, dp_parts).T

    grad_parts = attend_back(
        lengths, query_low, key_low, values_low, grad_context, logs, cos_table, sin_table
    )
    grad_qkv_low = jnp.concatenate(grad_parts, axis=1)
    grad_normed_one = tensor_collect(right_product(grad_qkv_low, full_qkv))
    total_qkv = low(left_product(rows_one, grad_qkv_low))
    grad_qkv = collect_blocks(total_qkv, dp_parts)
    norm_pull_one = jax.vjp(normalize, inputs)[1]
    input_grad = from_relative(grad_attended + norm_pull_one(grad_normed_one)[0])
    return (
        layer_output,
        input_grad,
        grad_qkv[:, :head_width],
        grad_qkv[:, head_width : 2 * head_width],
        grad_qkv[:, 2 * head_width :],
        grad_output,
        grad_gate,
        grad_up,
        grad_down,
    )


def solution(mesh):
    return jax.shard_map(
        shards,
        mesh=mesh,
        in_specs=(
            P(("dp", "tensor"), None),
            P("dp", "tensor"),
            P("dp", "tensor"),
            P("dp", "tensor"),
            P("tensor", "dp"),
            P("dp", "tensor"),
            P("dp", "tensor"),
            P("tensor", "dp"),
            P(("dp", "tensor"), None),
            P("dp"),
        ),
        out_specs=(
            P(("dp", "tensor"), None),
            P(("dp", "tensor"), None),
            P("dp", "tensor"),
            P("dp", "tensor"),
            P("dp", "tensor"),
            P("tensor", "dp"),
            P("dp", "tensor"),
            P("dp", "tensor"),
            P("tensor", "dp"),
        ),
        check_vma=False,
    )
```
